32 devices in a mesh: pipe: 2 (over core), tensor: 2 (over x), expert: 8 (over z, y).
Axes of the slice: x: 2, y: 2, z: 4, core: 2. Of those that a mesh axis runs over, the one named last changes fastest.
Arguments:
- tokens: bfloat16 [3, 384, 4096], P(None, 'expert', 'tensor'), may hold values from -36 to 36
- norm_gain: float32 [2, 4096], P('pipe'), may hold values from 0.1 to 1.9
- shared_gate: bfloat16 [2, 4096, 1024], P('pipe', 'expert', 'tensor'), may hold values from -0.09375 to 0.09375
- shared_up: bfloat16 [2, 4096, 1024], P('pipe', 'expert', 'tensor'), may hold values from -0.09375 to 0.09375
- shared_down: bfloat16 [2, 1024, 4096], P('pipe', 'tensor', 'expert'), may hold values from -0.1875 to 0.1875
- expert_gate: bfloat16 [2, 8, 4096, 1024], P('pipe', 'expert', None, 'tensor'), may hold values from -0.09375 to 0.09375
- expert_up: bfloat16 [2, 8, 4096, 1024], P('pipe', 'expert', None, 'tensor'), may hold values from -0.09375 to 0.09375
- expert_down: bfloat16 [2, 8, 1024, 4096], P('pipe', 'expert', 'tensor'), may hold values from -0.1875 to 0.1875
- expert_ids: int32 [2, 3, 384, 8], P('pipe', None, 'expert'), may hold values from 0 to 255, as said below
- expert_slots: int32 [2, 3, 384, 8], P('pipe', None, 'expert'), may hold values from -1 to 2, as said below
- route_weights: float32 [2, 3, 384, 8], P('pipe', None, 'expert'), may hold values from 0.1 to 1
Outputs:
- states: bfloat16 [2, 3, 384, 4096], P('pipe', None, 'expert', 'tensor')
The draws below stay inside these ranges and needn't reach their ends.
Inputs may be any that keep to these rules, and one draw needn't show every extreme that they name: `expert_ids`: the 8 ids of a token are distinct. Ids of 8 and above name experts that are not held and add nothing. `expert_slots`: for a choice whose id is below 8: the number of earlier choices (earlier tokens, or lower k of the same token) of the same block of 48 tokens, same layer and microbatch, that name the same expert, if that number is below 3; otherwise -1. For ids of 8 and above: -1.
All inputs are finite; a program needn't handle non-finite values.
Results may differ from the reference program's by a relative error of at most 0.0085.
Values may be sent and summed in bfloat16 or wider, within the bound.
A program may use at most 64 MiB of HBM per device.

```python
import math
import jax
import jax.numpy as jnp
from jax import lax

D = 4096
FE = 1024
FS = 1024
ROUTED = 256
TOP = 8
CAP = 3
TE = 48
MB = 3
LAYERS = 2
HELD = 8
FE_DEV = 512
TOKENS = 384
N_TENSOR = 2


def route_table(key):
    subkeys = jax.random.split(jax.random.fold_in(key, 7001), 4)
    blocks = TOKENS // TE
    jitter = jax.random.randint(subkeys[0], (LAYERS, MB, TOKENS, ROUTED), 0, 2 ** 20, dtype=jnp.int32)
    popular = jax.random.randint(subkeys[1], (LAYERS, MB, 1, ROUTED), 0, 2, dtype=jnp.int32) * 2 ** 17
    hot_expert = jax.random.randint(subkeys[2], (LAYERS, MB, 1, 1), 0, HELD, dtype=jnp.int32)
    shuffle = jax.random.randint(subkeys[3], (LAYERS, MB, blocks, TE), 0, 2 ** 30, dtype=jnp.int32)
    position = jnp.argsort(jnp.argsort(shuffle, axis=-1, stable=True), axis=-1, stable=True)
    forced = (position < CAP + 1).reshape(LAYERS, MB, TOKENS, 1)
    column = jnp.arange(ROUTED, dtype=jnp.int32)
    lifted = jnp.where(forced & (column == hot_expert), 2 ** 21, 0).astype(jnp.int32)
    scores = (jitter + popular + lifted) * ROUTED + column
    chosen = lax.top_k(scores, TOP)[1].astype(jnp.int32)
    flat = chosen.reshape(LAYERS, MB, blocks, TE * TOP)
    in_window = flat < HELD
    matches = ((flat[..., None] == jnp.arange(HELD, dtype=jnp.int32)) & in_window[..., None]).astype(jnp.int32)
    earlier = jnp.cumsum(matches, axis=-2) - matches
    counted = jnp.sum(earlier * matches, axis=-1)
    slot_rank = jnp.where(in_window & (counted < CAP), counted, -1).astype(jnp.int32)
    return (chosen, slot_rank.reshape(LAYERS, MB, TOKENS, TOP))


def draw_expert_ids(key, part):
    return route_table(key)[0]


def draw_expert_slots(key, part):
    return route_table(key)[1]


def draw_tokens(key, part):
    subkeys = jax.random.split(jax.random.fold_in(key, 31), 3)
    row_scale = jnp.exp(jax.random.uniform(subkeys[0], (MB, TOKENS, 1), jnp.float32, jnp.log(0.3), jnp.log(3.0)))
    column_scale = jnp.exp(jax.random.uniform(subkeys[1], (1, 1, D), jnp.float32, jnp.log(0.3), jnp.log(3.0)))
    entries = jnp.clip(jax.random.normal(subkeys[2], (MB, TOKENS, D), jnp.float32), -4.0, 4.0)
    return jnp.clip(entries * row_scale * column_scale, -36.0, 36.0).astype(jnp.bfloat16)


def steps_of(rng, shape, cuts, smallest, top_value):
    loudness, own = 1.0, jax.random.fold_in(rng, 6)
    for axis_at, blocks in cuts:
        heights = jnp.exp(jax.random.uniform(jax.random.fold_in(own, axis_at), (blocks,), jnp.float32, smallest / len(cuts), top_value / len(cuts)))
        loudness = loudness * jnp.repeat(heights, shape[axis_at] // blocks).reshape([-1 if axis == axis_at else 1 for axis in range(len(shape))])
    return loudness


def bell_draw(own_key, extent, spread, most, cuts=(), held_as=jnp.bfloat16):
    loudness = steps_of(own_key, extent, cuts, -0.22, 0.18) if cuts else 1.0
    array = jax.random.normal(own_key, extent, jnp.float32) * spread * loudness
    return jnp.minimum(jnp.maximum(array, -most), most).astype(held_as)


def setup_inputs(seed: int = 0) -> dict:
    key_of = jax.random.split(jax.random.key(seed), 12)
    return {
        "tokens": draw_tokens(jax.random.fold_in(key_of[11], 71), 0),
        "norm_gain": jnp.clip(1.0 + 0.18 * jax.random.normal(key_of[1], (LAYERS, D), jnp.float32), 0.1, 1.9),
        "shared_gate": bell_draw(key_of[2], (LAYERS, D, FS), D ** -0.5, 0.09375, ((0, 2), (1, 8), (2, 2))),
        "shared_up": bell_draw(key_of[3], (LAYERS, D, FS), D ** -0.5, 0.09375, ((0, 2), (1, 8), (2, 2))),
        "shared_down": bell_draw(key_of[4], (LAYERS, FS, D), FS ** -0.5, 0.1875, ((0, 2), (1, 2), (2, 8))),
        "expert_gate": bell_draw(key_of[5], (LAYERS, HELD, D, FE), D ** -0.5, 0.09375, ((0, 2), (1, 8), (3, 2))),
        "expert_up": bell_draw(key_of[6], (LAYERS, HELD, D, FE), D ** -0.5, 0.09375, ((0, 2), (1, 8), (3, 2))),
        "expert_down": bell_draw(key_of[7], (LAYERS, HELD, FE, D), FE ** -0.5, 0.1875, ((0, 2), (1, 8), (2, 2))),
        "expert_ids": draw_expert_ids(jax.random.fold_in(key_of[11], 71), 0),
        "expert_slots": draw_expert_slots(jax.random.fold_in(key_of[11], 71), 0),
        "route_weights": jnp.clip(jnp.exp(math.log(1.0) - 2.3025851 * jax.random.uniform(key_of[10], (LAYERS, MB, TOKENS, TOP), jnp.float32) ** steps_of(key_of[10], (LAYERS, MB, TOKENS, TOP), ((0, 2), (2, 8)), -0.2, 0.2)), 0.1, 1.0),
    }


def product(left, right):
    return jnp.dot(left, right, preferred_element_type=jnp.float32)

def apply_layer(state, gain, sh_gate, sh_up, sh_down, ex_gate, ex_up, ex_down, route_ids, slot_rank, weights):
    values = state.astype(jnp.float32)
    inverse_rms = lax.rsqrt(lax.optimization_barrier(jnp.mean(values * values, axis=-1, keepdims=True)) + 1e-06)
    normed = (values * inverse_rms * gain).astype(jnp.bfloat16)
    shared_hidden = (jax.nn.silu(product(normed, sh_gate)) * product(normed, sh_up)).astype(jnp.bfloat16)
    shared_out = product(shared_hidden, sh_down)
    valid = (route_ids < HELD) & (slot_rank >= 0)
    slot_code = jnp.where(valid, route_ids * CAP + slot_rank, -1).astype(jnp.int32)
    blocks = TOKENS // TE
    code_blocks = slot_code.reshape(blocks, TE, TOP)
    slot_range = jnp.arange(HELD * CAP, dtype=jnp.int32)
    picker = jnp.any(code_blocks[:, None, :, :] == slot_range[None, :, None, None], axis=3).astype(jnp.float32)
    buffers = jnp.einsum('bjt,btd->bjd', picker, normed.reshape(blocks, TE, D).astype(jnp.float32)).astype(jnp.bfloat16)
    expert_rows = buffers.reshape(blocks, HELD, CAP, D).transpose(1, 0, 2, 3).reshape(HELD, blocks * CAP, D)

    def one_expert(operands):
        rows, w_gate, w_up, w_down = operands
        hidden = (jax.nn.silu(product(rows, w_gate)) * product(rows, w_up)).astype(jnp.bfloat16)
        summed = jnp.zeros((rows.shape[0], D), jnp.float32)
        for group in range(N_TENSOR):
            part = product(hidden[:, group * FE_DEV:(group + 1) * FE_DEV], w_down[group * FE_DEV:(group + 1) * FE_DEV]).astype(jnp.bfloat16)
            part = lax.optimization_barrier(part)
            summed = summed + part.astype(jnp.float32)
        return summed
    outputs = lax.map(one_expert, (expert_rows, ex_gate, ex_up, ex_down))
    returned = outputs.reshape(HELD, blocks, CAP, D).transpose(1, 0, 2, 3).reshape(blocks, HELD * CAP, D)
    index = jnp.maximum(code_blocks, 0).reshape(blocks, TE * TOP)[:, :, None]
    picked = jnp.take_along_axis(returned, index, axis=1).reshape(TOKENS, TOP, D)
    route_share = jnp.where(slot_code >= 0, weights, jnp.float32(0.0))
    routed = lax.optimization_barrier(jnp.sum(route_share[:, :, None] * picked, axis=1))
    return (values + shared_out + routed).astype(jnp.bfloat16)

def reference(tokens, norm_gain, shared_gate, shared_up, shared_down, expert_gate, expert_up, expert_down, expert_ids, expert_slots, route_weights):
    states = []
    for layer_index in range(LAYERS):
        layer_out = []
        for batch_index in range(MB):
            if layer_index == 0:
                state = tokens[batch_index]
            else:
                state = states[layer_index - 1][batch_index]
            layer_out.append(apply_layer(state, norm_gain[layer_index], shared_gate[layer_index], shared_up[layer_index], shared_down[layer_index], expert_gate[layer_index], expert_up[layer_index], expert_down[layer_index], expert_ids[layer_index, batch_index], expert_slots[layer_index, batch_index], route_weights[layer_index, batch_index]))
        states.append(jnp.stack(layer_out))
    return jnp.stack(states)
```

```python
import functools

import jax
import jax.numpy as jnp
from jax import lax
from jax.experimental import pallas as pl
from jax.experimental.pallas import tpu as pltpu
from jax.sharding import PartitionSpec as P

CAP = 3
GROUP = 2
MESH = pl.DeviceIdType.MESH
F32 = jnp.float32
BF16 = jnp.bfloat16


def product(left, right):
    return jnp.dot(left, right, preferred_element_type=F32)


def silu(value):
    return value / (1.0 + jnp.exp(-value))


def layer_kernel(
    ne, nt, ng,
    x_hbm, gain, picker, combine, sg_hbm, su_hbm, sd_hbm, eg_hbm, eu_hbm, ed_hbm,
    out,
    xs, xr, sq, sqn, inv, xn, xg, sg, su, sd, eg, eu, ed,
    gs, gr, own_acc, hid, oy, oz,
    outg, arr, outc, ret, hy, hr, eg_acc, eu_acc, ehid, res,
    wx_send, wx_recv, wy_send, wy_recv, fx_send, fx_recv, fy_send, fy_recv,
    q_send, q_recv, q2_send, x_send, x_recv, p_send, p_recv, p2_send,
    s_send, s_recv, g_send, g_recv, n_send, n_recv, o_send, o_recv,
    a_send, a_recv, b_send, b_recv, f_send, f_recv, h_send, h_recv,
    own_sem, exp_sem, x_sem, go_sem,
):
    pipe = lax.axis_index("pipe")
    ten = lax.axis_index("tensor")
    me = lax.axis_index("expert")
    no = ne // ng
    spt = ne // nt
    opt = spt // ng
    grp = me // ng
    sub = me % ng
    T, Gs = xs.shape[1], xs.shape[2]
    R = xr.shape[1]
    step = (T - R) // max(nt - 1, 1)
    Ds, F = sg.shape[2], sg.shape[3]
    FS = nt * F
    rows = outg.shape[1]
    width = opt * Gs
    owner = grp // opt
    slot = grp % opt

    def remote(src, dst, send, recv, **device):
        return pltpu.make_async_remote_copy(
            src_ref=src, dst_ref=dst, send_sem=send, recv_sem=recv,
            device_id=device, device_id_type=MESH,
        )

    def far(d):
        return (grp + d) % no

    def expert_at(group):
        return group * ng + sub

    def tensor_at(k):
        return (ten + k) % nt

    def subset(k):
        return pl.ds(pl.multiple_of(k * step, 16), R)

    barrier = pltpu.get_barrier_semaphore()
    greeted = 0
    for k in range(1, ne):
        pl.semaphore_signal(barrier, inc=1, device_id={"expert": (me + k) % ne}, device_id_type=MESH)
        greeted += 1
    for k in range(1, nt):
        pl.semaphore_signal(barrier, inc=1, device_id={"tensor": tensor_at(k)}, device_id_type=MESH)
        greeted += 1
        for d in range(1, no):
            pl.semaphore_signal(
                barrier, inc=1, device_id={"tensor": tensor_at(k), "expert": expert_at(far(d))}, device_id_type=MESH
            )
            greeted += 1
    for k in range(nt):
        pl.semaphore_signal(
            barrier, inc=1, device_id={"pipe": 1 - pipe, "tensor": tensor_at(k)}, device_id_type=MESH
        )
        greeted += 1

    x_in = [
        pltpu.make_async_copy(x_hbm.at[:, pl.ds(i * Gs, Gs)], xs.at[i], x_sem.at[i])
        for i in range(opt)
    ]

    @pl.when(pipe == 0)
    def _():
        for copy in x_in:
            copy.start()

    own = [
        pltpu.make_async_copy(sg_hbm, sg.at[ten, sub], own_sem.at[0]),
        pltpu.make_async_copy(su_hbm, su.at[ten, sub], own_sem.at[1]),
        pltpu.make_async_copy(sd_hbm, sd.at[sub, ten], own_sem.at[2]),
    ]
    for copy in own:
        copy.start()
    experts = [
        pltpu.make_async_copy(eg_hbm, eg, exp_sem.at[0]),
        pltpu.make_async_copy(eu_hbm, eu, exp_sem.at[1]),
        pltpu.make_async_copy(ed_hbm, ed, exp_sem.at[2]),
    ]
    for copy in experts:
        copy.start()
    pl.semaphore_wait(barrier, greeted)

    def shard(w, t, j):
        if w == 2:
            return sd.at[j, t]
        return (sg, su)[w].at[t, j]

    cut = (Ds // 2, Ds // 2, F // 2)
    full = (Ds, Ds, F)

    def weight_x(w, k):
        block = shard(w, ten, sub)
        return remote(block, block, wx_send.at[w, k - 1], wx_recv.at[w, k - 1], tensor=tensor_at(k))

    def weight_y(w, r):
        block = shard(w, ten, sub)
        return remote(block, block, wy_send.at[w, r - 1], wy_recv.at[w, r - 1], expert=grp * ng + (sub + r) % ng)

    def forward_y(w, k, r):
        block = shard(w, (ten + nt - k) % nt, sub).at[pl.ds(0, cut[w])]
        return remote(
            block, block, fy_send.at[w, k - 1, r - 1], fy_recv.at[w, k - 1, r - 1],
            expert=grp * ng + (sub + r) % ng,
        )

    def forward_x(w, k, r):
        block = shard(w, ten, (sub + ng - r) % ng).at[pl.ds(cut[w], full[w] - cut[w])]
        return remote(
            block, block, fx_send.at[w, k - 1, r - 1], fx_recv.at[w, k - 1, r - 1], tensor=tensor_at(k)
        )

    def send_x(w):
        for k in range(1, nt):
            weight_x(w, k).start()

    def send_y(w):
        for r in range(1, ng):
            weight_y(w, r).start()

    def pass_x(w):
        for r in range(1, ng):
            weight_y(w, r).wait_recv()
            for k in range(1, nt):
                forward_x(w, k, r).start()

    def pass_y(w):
        for k in range(1, nt):
            weight_x(w, k).wait_recv()
            for r in range(1, ng):
                forward_y(w, k, r).start()

    def gathered(w):
        for k in range(1, nt):
            for r in range(1, ng):
                forward_x(w, k, r).wait_recv()
                forward_y(w, k, r).wait_recv()

    first = pipe == 0

    @pl.when(pipe == 1)
    def _():
        pl.semaphore_wait(go_sem, 1)

    def x_copy(k, i):
        return remote(
            xs.at[i, subset(tensor_at(k))], xr.at[ten * opt + i],
            x_send.at[k - 1, i], x_recv.at[k - 1, i], tensor=tensor_at(k),
        )

    def q_copy(k):
        return remote(sq.at[ten], sq.at[ten], q_send.at[k], q_recv.at[k], tensor=tensor_at(k))

    def squares(total):
        return jnp.broadcast_to(total, (T, sq.shape[2]))

    @pl.when(first)
    def _():
        total = jnp.zeros((T, 1), F32)
        for i in range(opt):
            x_in[i].wait()
            for k in range(1, nt):
                x_copy(k, i).start()
            v = xs[i].astype(F32)
            total += jnp.sum(v * v, axis=-1, keepdims=True)
        sq[ten] = squares(total)
        for k in range(1, nt):
            q_copy(k).start()

    for copy in own:
        copy.wait()

    @pl.when(first)
    def _():
        send_x(0)
        send_y(0)
        send_y(1)

    @pl.when(pipe == 1)
    def _():
        for w in range(3):
            send_x(w)
            send_y(w)
        for w in range(3):
            pass_x(w)
            pass_y(w)
        for w in range(3):
            gathered(w)
        for i in range(opt):
            remote(xs.at[i], xs.at[i], p_send.at[i], p_recv.at[i], pipe=1 - pipe).wait_recv()
        q_copy(0).wait_recv()

    for k in range(1, nt):
        q_copy(k).wait_recv()
    total = sq[0]
    for t in range(1, nt):
        total += sq[t]
    inv[...] = lax.rsqrt(total / (ne * Ds) + 1e-06)

    def spread_rows(o):
        return remote(xn.at[o], xg.at[grp], s_send.at[o], s_recv.at[grp], expert=expert_at(o))

    mine = inv[subset(ten), :1]

    def normed_rows(o, value):
        xn[o] = (value.astype(F32) * mine * gain[o]).astype(BF16)

        @pl.when(o != grp)
        def _():
            spread_rows(o).start()

    for i in range(opt):
        normed_rows(ten * opt + i, xs[i, subset(ten)])
    for k in range(1, nt):
        for i in range(opt):
            x_copy(k, i).wait_recv()
            o = ((ten + nt - k) % nt) * opt + i
            normed_rows(o, xr[o])

    def dispatch(k):
        to = (me + k) % ne
        return remote(outg.at[to], arr.at[ten, me], a_send.at[k - 1], a_recv.at[k - 1], expert=to)

    def spread(q, k):
        block = arr.at[ten, (me + ne - k) % ne]
        return remote(block, block, f_send.at[q - 1, k], f_recv.at[q - 1, k], tensor=tensor_at(q))

    def give_back(k):
        to = (me + k) % ne
        return remote(outc.at[to], ret.at[me], b_send.at[k - 1], b_recv.at[k - 1], expert=to)

    for i in range(opt):
        v = (xs[i].astype(F32) * inv[:, :1] * gain[ten * opt + i]).astype(BF16)
        for c in range(ng):
            sent = product(picker[...], v[:, c * Ds:(c + 1) * Ds]).astype(BF16)
            outg[:, :, i * Gs + c * Ds:i * Gs + (c + 1) * Ds] = sent.reshape(ne, rows, Ds)
    for k in range(1, ne):
        dispatch(k).start()
    arr[ten, me] = outg[me]

    @pl.when(first)
    def _():
        pass_x(0)
        send_x(1)
        pass_y(0)
        pass_x(1)
        gathered(0)

    def await_group(sem, o, ref):
        remote(ref, ref, sem, sem, expert=expert_at(o)).wait_recv()

    def partial(w, o):
        return remote(gs.at[w, o], gr.at[w, grp], g_send.at[w, o], g_recv.at[w, grp], expert=expert_at(o))

    def partials(w):
        weights = (sg, su)[w]
        for d in range(1, no):
            o = far(d)
            if w == 0:
                await_group(s_recv.at[o], o, xg.at[o])
            for t in range(nt):
                gs[w, o, :, t * F:(t + 1) * F] = product(xg[o], weights[t].reshape(Gs, F)).astype(BF16)
            partial(w, o).start()

    def own_partials(w):
        weights = (sg, su)[w]
        for t in range(nt):
            own_acc[w, :, t * F:(t + 1) * F] = product(xn[grp], weights[t].reshape(Gs, F))

    partials(0)

    @pl.when(first)
    def _():
        pass_y(1)
        gathered(1)

    partials(1)
    for q in range(1, nt):
        spread(q, 0).start()
    for k in range(1, ne):
        dispatch(k).wait_recv()
        for q in range(1, nt):
            spread(q, k).start()

    @pl.when(first)
    def _():
        send_x(2)
        send_y(2)

    own_partials(0)
    own_partials(1)

    for copy in experts:
        copy.wait()
    eg_acc[...] = jnp.zeros_like(eg_acc)
    eu_acc[...] = jnp.zeros_like(eu_acc)

    def expert_in(group):
        for i in range(spt):
            depth = pl.ds(pl.multiple_of(group * (spt * Ds) + i * Ds, 128), Ds)
            v = arr[group, :, :, i * Ds:(i + 1) * Ds].reshape(ne * rows, Ds)
            eg_acc[...] += product(v, eg[depth, :])
            eu_acc[...] += product(v, eu[depth, :])

    expert_in(ten)
    for q in range(1, nt):
        for k in range(ne):
            spread(q, k).wait_recv()
        expert_in((ten + q) % nt)
    ehid[...] = (silu(eg_acc[...]) * eu_acc[...]).astype(BF16)

    def h_copy(q, i):
        at = (q - 1) * spt + i
        return remote(hy.at[at], hr.at[at], h_send.at[at], h_recv.at[at], tensor=tensor_at(q))

    def expert_out(group, i):
        return product(ehid[...], ed[:, pl.ds(pl.multiple_of(group * (spt * Ds) + i * Ds, 128), Ds)])

    for q in range(1, nt):
        for i in range(spt):
            hy[(q - 1) * spt + i] = expert_out((ten + q) % nt, i).astype(BF16)
            h_copy(q, i).start()

    def hidden(o):
        return remote(hid.at[grp], hid.at[grp], n_send.at[o], n_recv.at[grp], expert=expert_at(o))

    for w in range(2):
        for d in range(1, no):
            o = far(d)
            await_group(g_recv.at[w, o], o, gr.at[w, o])
    g, u = own_acc[0], own_acc[1]
    for d in range(1, no):
        o = far(d)
        g += gr[0, o].astype(F32)
        u += gr[1, o].astype(F32)
    hid[grp] = (silu(g) * u).astype(BF16)
    for d in range(1, no):
        hidden(far(d)).start()

    @pl.when(first)
    def _():
        pass_x(2)
        pass_y(2)
        pl.semaphore_signal(go_sem, inc=1, device_id={"pipe": 1 - pipe}, device_id_type=MESH)

    for i in range(spt):
        value = expert_out(ten, i)
        for q in range(1, nt):
            h_copy(q, i).wait_recv()
            value += hr[(q - 1) * spt + i].astype(F32)
        outc[:, :, i * Ds:(i + 1) * Ds] = value.astype(BF16).reshape(ne, rows, Ds)
    for k in range(1, ne):
        give_back(k).start()
    ret[me] = outc[me]

    @pl.when(first)
    def _():
        gathered(2)

    def o_copy(o):
        return remote(
            oy.at[o], oz.at[slot, ten], o_send.at[o], o_recv.at[slot, ten], tensor=owner, expert=expert_at(o)
        )

    for d in list(range(1, no)) + [0]:
        o = far(d)
        if d > 0:
            await_group(n_recv.at[o], o, hid.at[o])
        for j in range(ng):
            oy[o, :, j * Ds:(j + 1) * Ds] = product(hid[o], sd[j].reshape(FS, Ds)).astype(BF16)
        if d > 0:
            o_copy(o).start()
        else:
            @pl.when(owner != ten)
            def _():
                o_copy(o).start()

            @pl.when(owner == ten)
            def _():
                oz[slot, ten] = oy[o]

    weights = combine[...]
    high = weights.astype(BF16)
    low = (weights - high.astype(F32)).astype(BF16)
    for k in range(1, ne):
        give_back(k).wait_recv()

    def raw_on(k, i):
        return remote(
            res.at[i, subset(tensor_at(k))], xr.at[ten * opt + i], p2_send.at[k - 1, i], x_recv.at[k - 1, i],
            pipe=1 - pipe, tensor=tensor_at(k),
        )

    def state_on(i):
        return remote(res.at[i], xs.at[i], p_send.at[i], p_recv.at[i], pipe=1 - pipe)

    def squares_on(k):
        return remote(sqn, sq.at[ten], q2_send.at[k], q_recv.at[k], pipe=1 - pipe, tensor=tensor_at(k))

    total = jnp.zeros((T, 1), F32)
    for i in range(opt):
        for s in range(nt):
            @pl.when((ten * opt + i != grp) | (s != ten))
            def _():
                remote(
                    oz.at[i, s], oz.at[i, s], o_recv.at[i, s], o_recv.at[i, s], tensor=(ten + 1) % nt
                ).wait_recv()

        v = ret[:, :, i * Gs:(i + 1) * Gs].reshape(ne * rows, Gs)
        value = xs[i].astype(F32) + (product(high, v) + product(low, v))
        value += jnp.concatenate(
            [oz[i, s, :(step if s + 1 < nt else T - s * step)] for s in range(nt)], axis=0
        ).astype(F32)
        value = value.astype(BF16)
        res[i] = value
        out[:, i * Gs:(i + 1) * Gs] = value

        @pl.when(first)
        def _():
            for k in range(1, nt):
                raw_on(k, i).start()
            state_on(i).start()

        wide = value.astype(F32)
        total += jnp.sum(wide * wide, axis=-1, keepdims=True)

    @pl.when(first)
    def _():
        sqn[...] = squares(total)
        for k in range(nt):
            squares_on(k).start()

    for w in range(3):
        for k in range(1, nt):
            weight_x(w, k).wait_send()
        for r in range(1, ng):
            weight_y(w, r).wait_send()
        for k in range(1, nt):
            for r in range(1, ng):
                forward_x(w, k, r).wait_send()
                forward_y(w, k, r).wait_send()
    for d in range(1, no):
        o = far(d)
        spread_rows(o).wait_send()
        partial(0, o).wait_send()
        partial(1, o).wait_send()
        hidden(o).wait_send()
        o_copy(o).wait_send()

    @pl.when(owner != ten)
    def _():
        o_copy(grp).wait_send()

    for k in range(1, ne):
        dispatch(k).wait_send()
        give_back(k).wait_send()
    for q in range(1, nt):
        for i in range(spt):
            h_copy(q, i).wait_send()
        for k in range(ne):
            spread(q, k).wait_send()

    @pl.when(first)
    def _():
        for k in range(1, nt):
            q_copy(k).wait_send()
            for i in range(opt):
                x_copy(k, i).wait_send()
                raw_on(k, i).wait_send()
        for i in range(opt):
            state_on(i).wait_send()
        for k in range(nt):
            squares_on(k).wait_send()


def per_device(
    tokens, norm_gain, shared_gate, shared_up, shared_down,
    expert_gate, expert_up, expert_down, expert_ids, expert_slots, route_weights,
):
    ne = lax.axis_size("expert")
    nt = lax.axis_size("tensor")
    batches, block, width = tokens.shape
    T = batches * block
    D = width * nt
    Ds = shared_gate.shape[1]
    F = shared_gate.shape[2]
    FE = expert_gate.shape[3]
    spt = ne // nt
    ng = GROUP
    no = ne // ng
    opt = spt // ng
    Gs = ng * Ds
    FS = nt * F
    step = T // nt // 16 * 16
    R = T - (nt - 1) * step
    rows = -(-batches * CAP // 16) * 16

    ids, slots, weights = expert_ids[0], expert_slots[0], route_weights[0]
    valid = (ids < ne) & (slots >= 0)
    batch = jnp.arange(batches, dtype=jnp.int32)[:, None, None]
    code = jnp.where(valid, ids * rows + batch * CAP + slots, -1).reshape(T, -1)
    matched = code[:, :, None] == jnp.arange(ne * rows, dtype=jnp.int32)[None, None, :]
    picker = jnp.any(matched, axis=1).T.astype(BF16)
    combine = jnp.sum(jnp.where(matched, weights.reshape(T, -1)[:, :, None], F32(0.0)), axis=1)

    vmem = pl.BlockSpec(memory_space=pltpu.VMEM)
    hbm = pl.BlockSpec(memory_space=pl.ANY)
    dma = pltpu.SemaphoreType.DMA
    others = max(nt - 1, 1)
    near = max(ng - 1, 1)
    out = pl.pallas_call(
        functools.partial(layer_kernel, ne, nt, ng),
        out_shape=jax.ShapeDtypeStruct((T, width), BF16),
        in_specs=[hbm, vmem, vmem, vmem] + [hbm] * 6,
        out_specs=vmem,
        scratch_shapes=[
            pltpu.VMEM((opt, T, Gs), BF16),
            pltpu.VMEM((no, R, Gs), BF16),
            pltpu.VMEM((nt, T, 128), F32),
            pltpu.VMEM((T, 128), F32),
            pltpu.VMEM((T, 128), F32),
            pltpu.VMEM((no, R, Gs), BF16),
            pltpu.VMEM((no, R, Gs), BF16),
            pltpu.VMEM((nt, ng, Ds, F), BF16),
            pltpu.VMEM((nt, ng, Ds, F), BF16),
            pltpu.VMEM((ng, nt, F, Ds), BF16),
            pltpu.VMEM((D, FE), BF16),
            pltpu.VMEM((D, FE), BF16),
            pltpu.VMEM((FE, D), BF16),
            pltpu.VMEM((2, no, R, FS), BF16),
            pltpu.VMEM((2, no, R, FS), BF16),
            pltpu.VMEM((2, R, FS), F32),
            pltpu.VMEM((no, R, FS), BF16),
            pltpu.VMEM((no, R, Gs), BF16),
            pltpu.VMEM((opt, nt, R, Gs), BF16),
            pltpu.VMEM((ne, rows, width), BF16),
            pltpu.VMEM((nt, ne, rows, width), BF16),
            pltpu.VMEM((ne, rows, width), BF16),
            pltpu.VMEM((ne, rows, width), BF16),
            pltpu.VMEM((others * spt, ne * rows, Ds), BF16),
            pltpu.VMEM((others * spt, ne * rows, Ds), BF16),
            pltpu.VMEM((ne * rows, FE), F32),
            pltpu.VMEM((ne * rows, FE), F32),
            pltpu.VMEM((ne * rows, FE), BF16),
            pltpu.VMEM((opt, T, Gs), BF16),
            dma((3, others)), dma((3, others)), dma((3, near)), dma((3, near)),
            dma((3, others, near)), dma((3, others, near)), dma((3, others, near)), dma((3, others, near)),
            dma((nt,)), dma((nt,)), dma((nt,)),
            dma((others, opt)), dma((others, opt)), dma((opt,)), dma((opt,)), dma((others, opt)),
            dma((no,)), dma((no,)), dma((2, no)), dma((2, no)),
            dma((no,)), dma((no,)), dma((no,)), dma((opt, nt)),
            dma((ne - 1,)), dma((ne - 1,)), dma((ne - 1,)), dma((ne - 1,)),
            dma((others, ne)), dma((others, ne)),
            dma((others * spt,)), dma((others * spt,)),
            dma((3,)), dma((3,)), dma((opt,)),
            pltpu.SemaphoreType.REGULAR,
        ],
        compiler_params=pltpu.CompilerParams(
            collective_id=0, has_side_effects=True, vmem_limit_bytes=60 * 1024 * 1024
        ),
    )(
        tokens.reshape(T, width), norm_gain[0].reshape(no, 1, Gs), picker, combine,
        shared_gate[0], shared_up[0], shared_down[0],
        expert_gate[0, 0], expert_up[0, 0], expert_down[0, 0],
    )
    return out.reshape(1, batches, block, width)


def solution(mesh):
    in_specs = (
        P(None, "expert", "tensor"),
        P("pipe", None),
        P("pipe", "expert", "tensor"),
        P("pipe", "expert", "tensor"),
        P("pipe", "tensor", "expert"),
        P("pipe", "expert", None, "tensor"),
        P("pipe", "expert", None, "tensor"),
        P("pipe", "expert", "tensor", None),
        P("pipe", None, "expert", None),
        P("pipe", None, "expert", None),
        P("pipe", None, "expert", None),
    )
    out_specs = P("pipe", None, "expert", "tensor")
    return jax.shard_map(
        per_device, mesh=mesh, in_specs=in_specs, out_specs=out_specs, check_vma=False
    )
```

```python
import functools

import jax
import jax.numpy as jnp
from jax import lax
from jax.experimental import pallas as pl
from jax.experimental.pallas import tpu as pltpu
from jax.sharding import PartitionSpec as P

CAP = 3
GROUP = 2
PACK = 8
MESH = pl.DeviceIdType.MESH
F32 = jnp.float32
BF16 = jnp.bfloat16


def product(left, right):
    return jnp.dot(left, right, preferred_element_type=F32)


def turned(left, right):
    return lax.dot_general(left, right, (((0,), (0,)), ((), ())), preferred_element_type=F32)


def silu(value):
    return value / (1.0 + jnp.exp(-value))


def layer_kernel(
    ne, nt, ng,
    x_hbm, gain, ids, slots, shares, sg_hbm, su_hbm, sd_hbm, eg_hbm, eu_hbm, ed_hbm,
    out,
    xs, xr, sq, sqn, inv, xn, xg, sg, su, sd, eg, eu, ed,
    gs, gr, own_acc, hid, oy, oz,
    pick_low, pick_high, pick_tail, comb_high, comb_low,
    outg, arr, outc, ret, er, rt, tails, hy, hr, eg_acc, eu_acc, ehid, res,
    wx_send, wx_recv, wy_send, wy_recv, fx_send, fx_recv, fy_send, fy_recv,
    q_send, q_recv, q2_send, x_send, x_recv, p_send, p_recv, p2_send,
    s_send, s_recv, g_send, g_recv, n_send, n_recv, o_send, o_recv,
    a_send, a_recv, b_send, b_recv, f_send, f_recv, h_send, h_recv,
    own_sem, exp_sem, x_sem, go_sem,
):
    pipe = lax.axis_index("pipe")
    ten = lax.axis_index("tensor")
    me = lax.axis_index("expert")
    no = ne // ng
    spt = ne // nt
    opt = spt // ng
    grp = me // ng
    sub = me % ng
    T, Gs = xs.shape[1], xs.shape[2]
    R = xr.shape[1]
    step = (T - R) // max(nt - 1, 1)
    Ds, F = sg.shape[2], sg.shape[3]
    FS = nt * F
    width = opt * Gs
    half = spt // 2
    wide = half * Ds
    lanes = tails.shape[1]
    chunks = Ds // lanes
    kept = rt.shape[0]
    batches, top, block = ids.shape
    owner = grp // opt
    slot = grp % opt

    def remote(src, dst, send, recv, **device):
        return pltpu.make_async_remote_copy(
            src_ref=src, dst_ref=dst, send_sem=send, recv_sem=recv,
            device_id=device, device_id_type=MESH,
        )

    def far(d):
        return (grp + d) % no

    def expert_at(group):
        return group * ng + sub

    def beside(r):
        return grp * ng + (sub + r) % ng

    def tensor_at(k):
        return (ten + k) % nt

    def subset(k):
        return pl.ds(pl.multiple_of(k * step, 16), R)

    barrier = pltpu.get_barrier_semaphore()
    greeted = 0
    for k in range(1, ne):
        pl.semaphore_signal(barrier, inc=1, device_id={"expert": (me + k) % ne}, device_id_type=MESH)
        greeted += 1
    for k in range(1, nt):
        pl.semaphore_signal(barrier, inc=1, device_id={"tensor": tensor_at(k)}, device_id_type=MESH)
        greeted += 1
        for d in range(1, no):
            pl.semaphore_signal(
                barrier, inc=1, device_id={"tensor": tensor_at(k), "expert": expert_at(far(d))}, device_id_type=MESH
            )
            greeted += 1
    for k in range(nt):
        pl.semaphore_signal(
            barrier, inc=1, device_id={"pipe": 1 - pipe, "tensor": tensor_at(k)}, device_id_type=MESH
        )
        greeted += 1

    x_in = [
        pltpu.make_async_copy(x_hbm.at[:, pl.ds(i * Gs, Gs)], xs.at[i], x_sem.at[i])
        for i in range(opt)
    ]

    @pl.when(pipe == 0)
    def _():
        for copy in x_in:
            copy.start()

    own = [
        pltpu.make_async_copy(sg_hbm, sg.at[ten, sub], own_sem.at[0]),
        pltpu.make_async_copy(su_hbm, su.at[ten, sub], own_sem.at[1]),
        pltpu.make_async_copy(sd_hbm, sd.at[sub, ten], own_sem.at[2]),
    ]
    for copy in own:
        copy.start()
    experts = [
        pltpu.make_async_copy(eg_hbm, eg, exp_sem.at[0]),
        pltpu.make_async_copy(eu_hbm, eu, exp_sem.at[1]),
        pltpu.make_async_copy(ed_hbm, ed, exp_sem.at[2]),
    ]
    for copy in experts:
        copy.start()
    pl.semaphore_wait(barrier, greeted)

    def shard(w, t, j):
        if w == 2:
            return sd.at[j, t]
        return (sg, su)[w].at[t, j]

    cut = (Ds // 2, Ds // 2, F // 2)
    full = (Ds, Ds, F)

    def piece(w, t, j, p):
        return shard(w, t, j).at[pl.ds(p * cut[w], cut[w] if p == 0 else full[w] - cut[w])]

    def weight_x(w, k, p):
        block = piece(w, ten, sub, p)
        return remote(block, block, wx_send.at[w, k - 1, p], wx_recv.at[w, k - 1, p], tensor=tensor_at(k))

    def weight_y(w, r, p):
        block = piece(w, ten, sub, p)
        return remote(block, block, wy_send.at[w, r - 1, p], wy_recv.at[w, r - 1, p], expert=beside(r))

    def forward_y(w, k, r):
        block = piece(w, (ten + nt - k) % nt, sub, 0)
        return remote(
            block, block, fy_send.at[w, k - 1, r - 1], fy_recv.at[w, k - 1, r - 1], expert=beside(r)
        )

    def forward_x(w, k, r):
        block = piece(w, ten, (sub + ng - r) % ng, 1)
        return remote(
            block, block, fx_send.at[w, k - 1, r - 1], fx_recv.at[w, k - 1, r - 1], tensor=tensor_at(k)
        )

    def send_x(w):
        for p in range(2):
            for k in range(1, nt):
                weight_x(w, k, p).start()

    def send_y(w, p):
        for r in range(1, ng):
            weight_y(w, r, p).start()

    def pass_x(w):
        for r in range(1, ng):
            weight_y(w, r, 1).wait_recv()
            for k in range(1, nt):
                forward_x(w, k, r).start()

    def pass_y(w):
        for k in range(1, nt):
            weight_x(w, k, 0).wait_recv()
            for r in range(1, ng):
                forward_y(w, k, r).start()

    def gathered(w):
        for k in range(1, nt):
            weight_x(w, k, 1).wait_recv()
        for r in range(1, ng):
            weight_y(w, r, 0).wait_recv()
        for k in range(1, nt):
            for r in range(1, ng):
                forward_x(w, k, r).wait_recv()
                forward_y(w, k, r).wait_recv()

    first = pipe == 0

    def x_copy(k, i):
        return remote(
            xs.at[i, subset(tensor_at(k))], xr.at[ten * opt + i],
            x_send.at[k - 1, i], x_recv.at[k - 1, i], tensor=tensor_at(k),
        )

    def q_copy(k):
        return remote(sq.at[ten], sq.at[ten], q_send.at[k], q_recv.at[k], tensor=tensor_at(k))

    def squares(total):
        return jnp.broadcast_to(total, (T, sq.shape[2]))

    @pl.when(first)
    def _():
        total = jnp.zeros((T, 1), F32)
        for i in range(opt):
            x_in[i].wait()
            v = xs[i].astype(F32)
            total += jnp.sum(v * v, axis=-1, keepdims=True)
        sq[ten] = squares(total)
        for k in range(1, nt):
            q_copy(k).start()
        for k in range(1, nt):
            for i in range(opt):
                x_copy(k, i).start()

    for copy in own:
        copy.wait()

    @pl.when(first)
    def _():
        send_x(0)
        send_y(0, 1)
        send_y(0, 0)
        send_y(1, 1)

    def rows_like(count):
        return lax.broadcasted_iota(jnp.int32, (count, block), 0)

    def marked(count, code, value):
        total = jnp.zeros((count, block), F32)
        for k in range(top):
            total = jnp.where(rows_like(count) == code[k:k + 1], value(k), total)
        return total

    for m in range(batches):
        held = (ids[m] < ne) & (slots[m] >= 0)
        place = slots[m] + m * CAP
        code = jnp.where(held & (place < PACK), ids[m] * (2 * PACK) + place, -2 * PACK)
        tail = jnp.where(held & (place >= PACK), ids[m], -1)
        back = jnp.where(place < PACK, ids[m] * PACK + place, ne * PACK + ids[m])
        back = jnp.where(held, back, -1)
        pick_low[m] = marked(pick_low.shape[1], code, lambda k: 1.0).astype(BF16)
        pick_high[m] = marked(pick_high.shape[1], code + PACK, lambda k: 1.0).astype(BF16)
        pick_tail[m] = marked(pick_tail.shape[1], tail, lambda k: 1.0).astype(BF16)
        share = marked(kept, back, lambda k: shares[m, k:k + 1, :])
        high = share.astype(BF16)
        comb_high[m] = high
        comb_low[m] = (share - high.astype(F32)).astype(BF16)

    @pl.when(pipe == 1)
    def _():
        pl.semaphore_wait(go_sem.at[0], 1)
        for w in range(2):
            send_y(w, 1)
            send_y(w, 0)
        pl.semaphore_wait(go_sem.at[1], 1)
        for w in range(2):
            send_x(w)
        for w in range(2):
            pass_x(w)
            pass_y(w)
        send_x(2)
        send_y(2, 1)
        send_y(2, 0)
        for w in range(2):
            gathered(w)
        for i in range(opt):
            remote(xs.at[i], xs.at[i], p_send.at[i], p_recv.at[i], pipe=1 - pipe).wait_recv()
        q_copy(0).wait_recv()

    for k in range(1, nt):
        q_copy(k).wait_recv()
    total = sq[0]
    for t in range(1, nt):
        total += sq[t]
    inv[...] = lax.rsqrt(total / (ne * Ds) + 1e-06)

    def spread_rows(o):
        return remote(xn.at[o], xg.at[grp], s_send.at[o], s_recv.at[grp], expert=expert_at(o))

    mine = inv[subset(ten), :1]

    def normed_rows(o, value):
        xn[o] = (value.astype(F32) * mine * gain[o]).astype(BF16)

        @pl.when(o != grp)
        def _():
            spread_rows(o).start()

    for i in range(opt):
        normed_rows(ten * opt + i, xs[i, subset(ten)])
    for k in range(1, nt):
        for i in range(opt):
            x_copy(k, i).wait_recv()
            o = ((ten + nt - k) % nt) * opt + i
            normed_rows(o, xr[o])

    def dispatch(k):
        to = (me + k) % ne
        return remote(outg.at[to], arr.at[ten, me], a_send.at[k - 1], a_recv.at[k - 1], expert=to)

    def spread(q, k):
        block = arr.at[ten, (me + ne - k) % ne]
        return remote(block, block, f_send.at[q - 1, k], f_recv.at[q - 1, k], tensor=tensor_at(q))

    def give_back(k):
        to = (me + k) % ne
        return remote(outc.at[to], ret.at[me], b_send.at[k - 1], b_recv.at[k - 1], expert=to)

    def own_normed(c):
        i, at = c * Ds // Gs, c * Ds % Gs
        column = gain[ten * opt + i]
        return (xs[i, :, at:at + Ds].astype(F32) * inv[:, :1] * column[:, at:at + Ds]).astype(BF16)

    def put_tail(c, value):
        for j in range(chunks):
            tails[pl.ds(c * chunks + j, ne, stride=2 * PACK), :] = value[:, j * lanes:(j + 1) * lanes]

    def packed_tails():
        return tails[...].reshape(ne, 2 * PACK, lanes).astype(BF16)

    def unpack(read, put):
        for c in range(half):
            both = read(c * Ds, Ds).astype(F32)
            put(0, ne * PACK, c * Ds, both[:, :PACK].reshape(ne * PACK, Ds))
            put(0, ne * PACK, wide + c * Ds, both[:, PACK:].reshape(ne * PACK, Ds))
        tails[...] = read(wide, lanes).astype(F32).reshape(ne * 2 * PACK, lanes)
        for c in range(spt * chunks):
            row = tails[pl.ds(c, ne, stride=2 * PACK), :]
            if kept > ne * PACK + ne:
                row = jnp.concatenate([row, jnp.zeros((kept - ne * PACK - ne, lanes), F32)], axis=0)
            put(ne * PACK, kept, c * lanes, row)

    tails[...] = jnp.zeros_like(tails)
    for c in range(half):
        v = (own_normed(c), own_normed(half + c))
        sent = jnp.zeros((ne * 2 * PACK, Ds), F32)
        last = [jnp.zeros((pick_tail.shape[1], Ds), F32)] * 2
        for m in range(batches):
            token = slice(m * block, (m + 1) * block)
            sent += product(pick_low[m], v[0][token]) + product(pick_high[m], v[1][token])
            if (m + 1) * CAP > PACK:
                last = [last[h] + product(pick_tail[m], v[h][token]) for h in range(2)]
        outg[:, :, c * Ds:(c + 1) * Ds] = sent.astype(BF16).reshape(ne, 2 * PACK, Ds)
        for h in range(2):
            put_tail(h * half + c, last[h][:ne])
    outg[:, :, wide:] = packed_tails()
    for k in range(1, ne):
        dispatch(k).start()
    arr[ten, me] = outg[me]

    @pl.when(first)
    def _():
        pass_x(0)
        send_x(1)
        pass_y(0)
        send_y(1, 0)
        pass_x(1)
        gathered(0)

    def await_group(sem, o, ref):
        remote(ref, ref, sem, sem, expert=expert_at(o)).wait_recv()

    def partial(w, o):
        return remote(gs.at[w, o], gr.at[w, grp], g_send.at[w, o], g_recv.at[w, grp], expert=expert_at(o))

    def partials(w):
        weights = (sg, su)[w]
        for d in range(1, no):
            o = far(d)
            if w == 0:
                await_group(s_recv.at[o], o, xg.at[o])
            for t in range(nt):
                gs[w, o, :, t * F:(t + 1) * F] = product(xg[o], weights[t].reshape(Gs, F)).astype(BF16)
            partial(w, o).start()

    def own_partials(w):
        weights = (sg, su)[w]
        for t in range(nt):
            own_acc[w, :, t * F:(t + 1) * F] = product(xn[grp], weights[t].reshape(Gs, F))

    partials(0)

    def spreading():
        for q in range(1, nt):
            spread(q, 0).start()
        for k in range(1, ne):
            dispatch(k).wait_recv()
            for q in range(1, nt):
                spread(q, k).start()

    @pl.when(first)
    def _():
        pass_y(1)
        spreading()
        send_x(2)
        send_y(2, 1)
        send_y(2, 0)
        gathered(1)
        pl.semaphore_signal(go_sem.at[0], inc=1, device_id={"pipe": 1 - pipe}, device_id_type=MESH)

    partials(1)

    @pl.when(pipe == 1)
    def _():
        spreading()

    own_partials(0)
    own_partials(1)

    for copy in experts:
        copy.wait()
    eg_acc[...] = jnp.zeros_like(eg_acc)
    eu_acc[...] = jnp.zeros_like(eu_acc)

    def expert_in(group):
        def put(begin, end, column, value):
            er[begin:end, column:column + value.shape[1]] = value.astype(BF16)

        unpack(lambda column, count: arr[group, :, :, column:column + count], put)
        for i in range(spt):
            depth = pl.ds(pl.multiple_of(group * (spt * Ds) + i * Ds, 128), Ds)
            v = er[:, i * Ds:(i + 1) * Ds]
            eg_acc[...] += product(v, eg[depth, :])
            eu_acc[...] += product(v, eu[depth, :])

    expert_in(ten)
    pass_x(2)
    for q in range(1, nt):
        for k in range(ne):
            spread(q, k).wait_recv()
        expert_in((ten + q) % nt)
    ehid[...] = (silu(eg_acc[...]) * eu_acc[...]).astype(BF16)

    def h_copy(q, i):
        at = (q - 1) * spt + i
        return remote(hy.at[at], hr.at[at], h_send.at[at], h_recv.at[at], tensor=tensor_at(q))

    def expert_out(group, i):
        return product(ehid[...], ed[:, pl.ds(pl.multiple_of(group * (spt * Ds) + i * Ds, 128), Ds)])

    for q in range(1, nt):
        for i in range(spt):
            hy[(q - 1) * spt + i] = expert_out((ten + q) % nt, i).astype(BF16)
            h_copy(q, i).start()

    pass_y(2)

    def hidden(o):
        return remote(hid.at[grp], hid.at[grp], n_send.at[o], n_recv.at[grp], expert=expert_at(o))

    for w in range(2):
        for d in range(1, no):
            o = far(d)
            await_group(g_recv.at[w, o], o, gr.at[w, o])
    g, u = own_acc[0], own_acc[1]
    for d in range(1, no):
        o = far(d)
        g += gr[0, o].astype(F32)
        u += gr[1, o].astype(F32)
    hid[grp] = (silu(g) * u).astype(BF16)
    for d in range(1, no):
        hidden(far(d)).start()

    def expert_sum(i):
        value = expert_out(ten, i)
        for q in range(1, nt):
            h_copy(q, i).wait_recv()
            value += hr[(q - 1) * spt + i].astype(F32)
        put_tail(i, value[ne * PACK:ne * PACK + ne])
        return value[:ne * PACK].reshape(ne, PACK, Ds)

    tails[...] = jnp.zeros_like(tails)
    for c in range(half):
        both = jnp.concatenate([expert_sum(c), expert_sum(half + c)], axis=1)
        outc[:, :, c * Ds:(c + 1) * Ds] = both.astype(BF16)
    outc[:, :, wide:] = packed_tails()
    for k in range(1, ne):
        give_back(k).start()
    ret[me] = outc[me]

    @pl.when(first)
    def _():
        pl.semaphore_signal(go_sem.at[1], inc=1, device_id={"pipe": 1 - pipe}, device_id_type=MESH)

    gathered(2)

    def o_copy(o):
        return remote(
            oy.at[o], oz.at[slot, ten], o_send.at[o], o_recv.at[slot, ten], tensor=owner, expert=expert_at(o)
        )

    for d in list(range(1, no)) + [0]:
        o = far(d)
        if d > 0:
            await_group(n_recv.at[o], o, hid.at[o])
        for j in range(ng):
            oy[o, :, j * Ds:(j + 1) * Ds] = product(hid[o], sd[j].reshape(FS, Ds)).astype(BF16)
        if d > 0:
            o_copy(o).start()
        else:
            @pl.when(owner != ten)
            def _():
                o_copy(o).start()

            @pl.when(owner == ten)
            def _():
                oz[slot, ten] = oy[o]

    for k in range(1, ne):
        give_back(k).wait_recv()

    def put_back(begin, end, column, value):
        rt[begin:end, column:column + value.shape[1]] = value.astype(BF16)

    unpack(lambda column, count: ret[:, :, column:column + count], put_back)

    def routed(i):
        v = rt[:, i * Gs:(i + 1) * Gs]
        return jnp.concatenate(
            [turned(comb_high[m], v) + turned(comb_low[m], v) for m in range(batches)], axis=0
        )

    def raw_on(k, i):
        return remote(
            res.at[i, subset(tensor_at(k))], xr.at[ten * opt + i], p2_send.at[k - 1, i], x_recv.at[k - 1, i],
            pipe=1 - pipe, tensor=tensor_at(k),
        )

    def state_on(i):
        return remote(res.at[i], xs.at[i], p_send.at[i], p_recv.at[i], pipe=1 - pipe)

    def squares_on(k):
        return remote(sqn, sq.at[ten], q2_send.at[k], q_recv.at[k], pipe=1 - pipe, tensor=tensor_at(k))

    total = jnp.zeros((T, 1), F32)
    for i in range(opt):
        for s in range(nt):
            @pl.when((ten * opt + i != grp) | (s != ten))
            def _():
                remote(
                    oz.at[i, s], oz.at[i, s], o_recv.at[i, s], o_recv.at[i, s], tensor=(ten + 1) % nt
                ).wait_recv()

        value = xs[i].astype(F32) + routed(i)
        value += jnp.concatenate(
            [oz[i, s, :(step if s + 1 < nt else T - s * step)] for s in range(nt)], axis=0
        ).astype(F32)
        value = value.astype(BF16)
        res[i] = value
        out[:, i * Gs:(i + 1) * Gs] = value

        @pl.when(first)
        def _():
            state_on(i).start()

        rounded = value.astype(F32)
        total += jnp.sum(rounded * rounded, axis=-1, keepdims=True)

    @pl.when(first)
    def _():
        sqn[...] = squares(total)
        for k in range(nt):
            squares_on(k).start()
        for k in range(1, nt):
            for i in range(opt):
                raw_on(k, i).start()

    for w in range(3):
        for p in range(2):
            for k in range(1, nt):
                weight_x(w, k, p).wait_send()
            for r in range(1, ng):
                weight_y(w, r, p).wait_send()
        for k in range(1, nt):
            for r in range(1, ng):
                forward_x(w, k, r).wait_send()
                forward_y(w, k, r).wait_send()
    for d in range(1, no):
        o = far(d)
        spread_rows(o).wait_send()
        partial(0, o).wait_send()
        partial(1, o).wait_send()
        hidden(o).wait_send()
        o_copy(o).wait_send()

    @pl.when(owner != ten)
    def _():
        o_copy(grp).wait_send()

    for k in range(1, ne):
        dispatch(k).wait_send()
        give_back(k).wait_send()
    for q in range(1, nt):
        for i in range(spt):
            h_copy(q, i).wait_send()
        for k in range(ne):
            spread(q, k).wait_send()

    @pl.when(first)
    def _():
        for k in range(1, nt):
            q_copy(k).wait_send()
            for i in range(opt):
                x_copy(k, i).wait_send()
                raw_on(k, i).wait_send()
        for i in range(opt):
            state_on(i).wait_send()
        for k in range(nt):
            squares_on(k).wait_send()


def per_device(
    tokens, norm_gain, shared_gate, shared_up, shared_down,
    expert_gate, expert_up, expert_down, expert_ids, expert_slots, route_weights,
):
    ne = lax.axis_size("expert")
    nt = lax.axis_size("tensor")
    batches, block, width = tokens.shape
    assert PACK <= batches * CAP <= PACK + 1
    T = batches * block
    D = width * nt
    Ds = shared_gate.shape[1]
    F = shared_gate.shape[2]
    FE = expert_gate.shape[3]
    spt = ne // nt
    ng = GROUP
    no = ne // ng
    opt = spt // ng
    Gs = ng * Ds
    FS = nt * F
    step = T // nt // 16 * 16
    R = T - (nt - 1) * step
    lanes = 128
    packed = width // 2 + lanes
    spare = -(-ne // 16) * 16
    kept = ne * PACK + spare

    vmem = pl.BlockSpec(memory_space=pltpu.VMEM)
    hbm = pl.BlockSpec(memory_space=pl.ANY)
    dma = pltpu.SemaphoreType.DMA
    others = max(nt - 1, 1)
    near = max(ng - 1, 1)
    out = pl.pallas_call(
        functools.partial(layer_kernel, ne, nt, ng),
        out_shape=jax.ShapeDtypeStruct((T, width), BF16),
        in_specs=[hbm, vmem, vmem, vmem, vmem] + [hbm] * 6,
        out_specs=vmem,
        scratch_shapes=[
            pltpu.VMEM((opt, T, Gs), BF16),
            pltpu.VMEM((no, R, Gs), BF16),
            pltpu.VMEM((nt, T, 128), F32),
            pltpu.VMEM((T, 128), F32),
            pltpu.VMEM((T, 128), F32),
            pltpu.VMEM((no, R, Gs), BF16),
            pltpu.VMEM((no, R, Gs), BF16),
            pltpu.VMEM((nt, ng, Ds, F), BF16),
            pltpu.VMEM((nt, ng, Ds, F), BF16),
            pltpu.VMEM((ng, nt, F, Ds), BF16),
            pltpu.VMEM((D, FE), BF16),
            pltpu.VMEM((D, FE), BF16),
            pltpu.VMEM((FE, D), BF16),
            pltpu.VMEM((2, no, R, FS), BF16),
            pltpu.VMEM((2, no, R, FS), BF16),
            pltpu.VMEM((2, R, FS), F32),
            pltpu.VMEM((no, R, FS), BF16),
            pltpu.VMEM((no, R, Gs), BF16),
            pltpu.VMEM((opt, nt, R, Gs), BF16),
            pltpu.VMEM((batches, ne * 2 * PACK, block), BF16),
            pltpu.VMEM((batches, ne * 2 * PACK, block), BF16),
            pltpu.VMEM((batches, spare, block), BF16),
            pltpu.VMEM((batches, kept, block), BF16),
            pltpu.VMEM((batches, kept, block), BF16),
            pltpu.VMEM((ne, 2 * PACK, packed), BF16),
            pltpu.VMEM((nt, ne, 2 * PACK, packed), BF16),
            pltpu.VMEM((ne, 2 * PACK, packed), BF16),
            pltpu.VMEM((ne, 2 * PACK, packed), BF16),
            pltpu.VMEM((kept, width), BF16),
            pltpu.VMEM((kept, width), BF16),
            pltpu.VMEM((ne * 2 * PACK, lanes), F32),
            pltpu.VMEM((others * spt, kept, Ds), BF16),
            pltpu.VMEM((others * spt, kept, Ds), BF16),
            pltpu.VMEM((kept, FE), F32),
            pltpu.VMEM((kept, FE), F32),
            pltpu.VMEM((kept, FE), BF16),
            pltpu.VMEM((opt, T, Gs), BF16),
            dma((3, others, 2)), dma((3, others, 2)), dma((3, near, 2)), dma((3, near, 2)),
            dma((3, others, near)), dma((3, others, near)), dma((3, others, near)), dma((3, others, near)),
            dma((nt,)), dma((nt,)), dma((nt,)),
            dma((others, opt)), dma((others, opt)), dma((opt,)), dma((opt,)), dma((others, opt)),
            dma((no,)), dma((no,)), dma((2, no)), dma((2, no)),
            dma((no,)), dma((no,)), dma((no,)), dma((opt, nt)),
            dma((ne - 1,)), dma((ne - 1,)), dma((ne - 1,)), dma((ne - 1,)),
            dma((others, ne)), dma((others, ne)),
            dma((others * spt,)), dma((others * spt,)),
            dma((3,)), dma((3,)), dma((opt,)),
            pltpu.SemaphoreType.REGULAR((2,)),
        ],
        compiler_params=pltpu.CompilerParams(
            collective_id=0, has_side_effects=True, vmem_limit_bytes=60 * 1024 * 1024
        ),
    )(
        tokens.reshape(T, width), norm_gain[0].reshape(no, 1, Gs),
        *(array[0].transpose(0, 2, 1) for array in (expert_ids, expert_slots, route_weights)),
        shared_gate[0], shared_up[0], shared_down[0],
        expert_gate[0, 0], expert_up[0, 0], expert_down[0, 0],
    )
    return out.reshape(1, batches, block, width)


def solution(mesh):
    in_specs = (
        P(None, "expert", "tensor"),
        P("pipe", None),
        P("pipe", "expert", "tensor"),
        P("pipe", "expert", "tensor"),
        P("pipe", "tensor", "expert"),
        P("pipe", "expert", None, "tensor"),
        P("pipe", "expert", None, "tensor"),
        P("pipe", "expert", "tensor", None),
        P("pipe", None, "expert", None),
        P("pipe", None, "expert", None),
        P("pipe", None, "expert", None),
    )
    out_specs = P("pipe", None, "expert", "tensor")
    return jax.shard_map(
        per_device, mesh=mesh, in_specs=in_specs, out_specs=out_specs, check_vma=False
    )
```
